32 devices in a mesh: owner: 16 (over z, x, core), rep: 2 (over y).
Axes of the slice: x: 2, y: 2, z: 4, core: 2. Of those that a mesh axis runs over, the one named last changes fastest.
Arguments:
- features: float32 [16384, 256], P(('owner', 'rep')), may hold values from -6 to 6
- group_ids: int32 [16384], P(('owner', 'rep')), may hold values from 0 to 65535, as said below
- survive: int32 [16384], P(('owner', 'rep')), may hold values from 0 to 1
- home_row: int32 [65536], replicated, may hold values from 0 to 65535, as said below
- hot_ids: int32 [256], replicated, may hold values from 0 to 65535, as said below
Outputs:
- group_out: float32 [65536, 256], P(('owner', 'rep'))
- group_count: float32 [65536], P(('owner', 'rep'))
- hot_out: float32 [256, 256], P('rep')
- hot_count: float32 [256], P('rep')
The draws below stay inside these ranges and needn't reach their ends.
Inputs may be any that keep to these rules, and one draw needn't show every extreme that they name: home_row is a permutation of the groups. hot_ids holds 256 different groups. `group_ids`: among the rows of one device, 128 name hot groups, and at most 64 rows name non-hot groups g whose home_row[g] // 4096 is one and the same owner index; on every device some owners get exactly 64 such rows.
All inputs are finite; a program needn't handle non-finite values.
Results may differ from the reference program's by a relative error of at most 0.00007.
Values sent between devices are 32-bit elements; how exact they have to be, the bound alone decides.
A program may use at most 64 MiB of HBM per device.

```python
import jax
import jax.numpy as jnp

F = 256
GROUPS = 65536
HOT = 256
ROWS_DEV = 512
ROWS = 16384
OWN_GROUPS = 4096
CAP = 64
HOT_ROWS = 128
N_OWNER = 16
DEVICES = 32


def shared_tables(key):
    home = jax.random.permutation(jax.random.fold_in(key, 11), GROUPS).astype(jnp.int32)
    inverse = jnp.zeros((GROUPS,), jnp.int32).at[home].set(jnp.arange(GROUPS, dtype=jnp.int32))
    index = jnp.arange(HOT, dtype=jnp.int32)
    hot = inverse[index % N_OWNER * OWN_GROUPS + OWN_GROUPS - 1 - index // N_OWNER]
    return (home, inverse, hot)


def draw_home_row(key, part):
    return shared_tables(key)[0]


def draw_hot_ids(key, part):
    return shared_tables(key)[2]


def row_layout(key):
    home, inverse, hot = shared_tables(key)
    cold_rows = ROWS_DEV - HOT_ROWS
    span = OWN_GROUPS - HOT // N_OWNER
    chosen = jax.random.randint(jax.random.fold_in(key, 31), (), 0, N_OWNER).astype(jnp.int32)

    def one_device(dev_key):
        keys = jax.random.split(dev_key, 6)
        limit = jax.random.randint(keys[0], (HOT_ROWS,), 1, HOT + 1)
        pick = jax.random.randint(keys[1], (HOT_ROWS,), 0, 1 << 20) % limit
        hot_part = hot[pick]
        shuffled = jax.random.permutation(keys[2], N_OWNER).astype(jnp.int32)
        where_chosen = jnp.argmax((shuffled == chosen).astype(jnp.int32)).astype(jnp.int32)
        first = shuffled[0]
        owners = shuffled.at[where_chosen].set(first).at[0].set(chosen)
        owner = owners[jnp.arange(cold_rows, dtype=jnp.int32) // CAP]
        limit_cold = jax.random.randint(keys[3], (cold_rows,), 1, span + 1)
        within = jax.random.randint(keys[4], (cold_rows,), 0, 1 << 20) % limit_cold
        cold_part = inverse[owner * OWN_GROUPS + within]
        ids = jnp.concatenate([hot_part, cold_part]).astype(jnp.int32)
        flagged = jnp.concatenate([jnp.zeros((HOT_ROWS,), jnp.int32), (owner == chosen).astype(jnp.int32)])
        order = jax.random.permutation(keys[5], ROWS_DEV)
        return (ids[order], flagged[order])
    dev_keys = jax.random.split(jax.random.fold_in(key, 23), DEVICES)
    ids, flagged = jax.vmap(one_device)(dev_keys)
    return (ids.astype(jnp.int32), flagged.astype(jnp.int32))


def draw_group_ids(key, part):
    return row_layout(key)[0].reshape(-1).astype(jnp.int32)


def draw_survive(key, part):
    flagged = row_layout(key)[1]
    coin = jax.random.randint(jax.random.fold_in(key, 41), (DEVICES, ROWS_DEV), 0, 2).astype(jnp.int32)
    full_device = jax.random.randint(jax.random.fold_in(key, 43), (DEVICES,), 0, 16) == 0
    alive = jnp.where((flagged == 1) | full_device[:, None], 1, coin)
    return alive.reshape(-1).astype(jnp.int32)


def level_of(own_key, extent, cuts, low, largest):
    def one(axis_at, parts):
        heights = jax.random.uniform(jax.random.fold_in(jax.random.fold_in(own_key, 6), axis_at), (parts,), jnp.float32, low / len(cuts), largest / len(cuts))
        return jnp.repeat(jnp.exp(heights), extent[axis_at] // parts).reshape((-1,) + (1,) * (len(extent) - axis_at - 1))

    level = one(*cuts[0])
    for cut in cuts[1:]:
        level = level * one(*cut)
    return level


def bell_draw(rng, shape, deviation, most, cuts=(), kind=jnp.bfloat16):
    factor_of = level_of(rng, shape, cuts, -0.22, 0.18) if cuts else 1.0
    drawn = jax.random.normal(rng, shape, jnp.float32) * deviation * factor_of
    return jnp.minimum(jnp.maximum(drawn, -most), most).astype(kind)


def setup_inputs(seed: int = 0) -> dict:
    arg_keys = jax.random.split(jax.random.key(seed), 6)
    features = bell_draw(arg_keys[0], (ROWS, F), 1.0, 6.0, ((0, 32),), jnp.float32)
    group_ids = draw_group_ids(jax.random.fold_in(arg_keys[5], 71), 0)
    survive = draw_survive(jax.random.fold_in(arg_keys[5], 71), 0)
    home_row = draw_home_row(jax.random.fold_in(arg_keys[5], 71), 0)
    hot_ids = draw_hot_ids(jax.random.fold_in(arg_keys[5], 71), 0)
    return {"features": features, "group_ids": group_ids, "survive": survive, "home_row": home_row, "hot_ids": hot_ids}


def reference(features, group_ids, survive, home_row, hot_ids):
    weight = jnp.where(survive == 1, 1.0, 0.0).astype(jnp.float32)
    hot_slot = jnp.zeros((GROUPS,), jnp.int32).at[hot_ids].set(jnp.arange(1, HOT + 1, dtype=jnp.int32))
    hot_of_row = hot_slot[group_ids]
    kept = features * weight[:, None]
    cold_target = jnp.where(hot_of_row > 0, GROUPS, home_row[group_ids]).astype(jnp.int32)
    hot_target = jnp.where(hot_of_row > 0, hot_of_row - 1, HOT).astype(jnp.int32)
    cold_sum = jax.ops.segment_sum(kept, cold_target, num_segments=GROUPS + 1)[:GROUPS]
    cold_count = jax.ops.segment_sum(weight, cold_target, num_segments=GROUPS + 1)[:GROUPS]
    hot_sum = jax.ops.segment_sum(kept, hot_target, num_segments=HOT + 1)[:HOT]
    hot_count = jax.ops.segment_sum(weight, hot_target, num_segments=HOT + 1)[:HOT]
    group_out = cold_sum / jnp.sqrt(1.0 + cold_count)[:, None]
    hot_out = hot_sum / jnp.sqrt(1.0 + hot_count)[:, None]
    return (group_out, cold_count, hot_out, hot_count)
```

```python
import functools

import jax
import jax.numpy as jnp
from jax import lax
from jax.experimental import pallas as pl
from jax.experimental.pallas import tpu as pltpu
from jax.sharding import PartitionSpec as P

MESH = pl.DeviceIdType.MESH
LANES = 128
SUB = 8
BF = jnp.bfloat16
F32 = jnp.float32


def iota(shape, axis):
    return lax.broadcasted_iota(jnp.int32, shape, axis)


def mm(a, b, dims=((1,), (0,))):
    return lax.dot_general(a, b, (dims, ((), ())), preferred_element_type=F32)


def split(x):
    hi = x.astype(BF)
    return hi, (x - hi.astype(F32)).astype(BF)


def onehot(mask):
    return jnp.where(mask, 1.0, 0.0).astype(BF)


def log2(n):
    return n.bit_length() - 1


class Sizes:
    def __init__(self, owners, reps, rows, width, groups, hots):
        self.owners, self.reps, self.rows, self.width, self.hots = owners, reps, rows, width, hots
        self.groups = groups
        self.own_groups = groups // owners
        self.home_dev = self.own_groups // reps
        self.cap = 2 * rows // owners
        self.nb = width // self.cap
        self.pair = LANES // self.cap
        self.pairs = owners // self.pair
        self.chips = owners // 2
        self.part = hots // reps // 2
        self.near = min(self.chips // 2, self.part // SUB)
        self.far = self.chips // self.near
        self.piece = self.part // self.near
        self.home_rows = self.home_dev // LANES


def kernel(
    s,
    ids_hbm,
    survive_hbm,
    hot_hbm,
    table_hbm,
    feat_hbm,
    sum_ref,
    count_ref,
    hot_sum_ref,
    hot_count_ref,
    ids_ref,
    survive_ref,
    hot_ref,
    table_ref,
    feat_ref,
    bucket,
    arrived,
    tags,
    tags_in,
    scale_ref,
    hot_part,
    hot_l1,
    hot_s1,
    hot_l2,
    hot_s2,
    hot_l3,
    hot_s3,
    hot_l4,
    hot_s4,
    hot_all,
    half_ref,
    halves_ref,
    load,
    send1,
    recv1,
    send2,
    recv2,
    tsend,
    trecv,
    tsend2,
    trecv2,
    hsend,
    h_core,
    h_near,
    h_rep,
    h_far,
    h_all,
    h_last,
    h_half,
):
    owners, reps, cap, nb = s.owners, s.reps, s.cap, s.nb
    rows, width, hots = s.rows, s.width, s.hots
    me = lax.axis_index("owner")
    rep = lax.axis_index("rep")
    core = lax.rem(me, 2)
    near = lax.rem(me // 2, s.near)

    loads = [
        pltpu.make_async_copy(src, dst, load.at[i])
        for i, (src, dst) in enumerate(
            (
                (table_hbm, table_ref),
                (ids_hbm, ids_ref),
                (survive_hbm, survive_ref),
                (hot_hbm, hot_ref),
                (feat_hbm, feat_ref),
            )
        )
    ]
    for copy in loads:
        copy.start()

    barrier = pltpu.get_barrier_semaphore()

    @pl.loop(1, owners)
    def _(d):
        pl.semaphore_signal(
            barrier, inc=1, device_id=(lax.rem(me + d, owners), rep), device_id_type=MESH
        )

    @pl.loop(1, reps)
    def _(d):
        pl.semaphore_signal(
            barrier, inc=1, device_id=(me, lax.rem(rep + d, reps)), device_id_type=MESH
        )

    flips = []
    bit = 1
    while bit < owners:
        flips.append((bit, bit - 2 * bit * lax.rem(me // bit, 2)))
        bit *= 2

    def partner(p):
        out = me
        for bit, flip in flips:
            if p & bit:
                out = out + flip
        return out

    def other_rep(q):
        return lax.rem(rep + q, reps)

    def remote(src, dst, send, recv, device):
        return pltpu.make_async_remote_copy(
            src_ref=src,
            dst_ref=dst,
            send_sem=send,
            recv_sem=recv,
            device_id=device,
            device_id_type=MESH,
        )

    for copy in loads[:4]:
        copy.wait()
    ids = ids_ref[...]
    live_f = jnp.where(survive_ref[...] == 1, 1.0, 0.0)
    table = table_ref[...]
    trows = table.shape[0]
    halves = jnp.concatenate([table >> 8, table & 255], axis=1).astype(F32).astype(BF)
    pick = onehot(iota((trows, rows), 0) == (ids >> 7))
    both = mm(halves, pick, ((0,), (0,)))
    column = both[:LANES] * 256.0 + both[LANES:]
    home = jnp.sum(
        jnp.where(iota((LANES, rows), 0) == (ids & (LANES - 1)), column, 0.0), axis=0, keepdims=True
    )
    target = jnp.floor(home * (1.0 / s.own_groups))
    label = home - target * s.own_groups + 1.0
    place_at = target.astype(jnp.int32) ^ me

    at = iota((hots, hots), 0)
    block = at >> log2(s.piece)
    number = (
        (block & (reps - 1)) * (2 * s.part)
        + (block >> log2(reps)) * s.piece
        + (at & (s.piece - 1))
    )
    hot_col = jnp.sum(
        jnp.where(number == iota((hots, hots), 1), hot_ref[...].astype(F32), 0.0),
        axis=1,
        keepdims=True,
    )
    matches = jnp.where(hot_col == ids.astype(F32), 1.0, 0.0)
    is_hot = jnp.max(matches, axis=0, keepdims=True)
    keep = live_f * (1.0 - is_hot)
    place_at = jnp.where(keep > 0.0, place_at, -1)

    member = jnp.where(iota((owners, rows), 0) == place_at, 1.0, 0.0)
    before = onehot(iota((rows, rows), 0) < iota((rows, rows), 1))
    position = mm(member.astype(BF), before)
    placed = jnp.sum(position * member, axis=0, keepdims=True).astype(jnp.int32)
    slot = jnp.where(keep > 0.0, place_at * cap + placed, -1)

    def make_tags():
        lane = placed + cap * (place_at & (s.pair - 1))
        label_hi = jnp.floor(label * (1.0 / 256.0))
        label_lo = label - 256.0 * label_hi
        coded = jnp.concatenate([member * label_hi, member * label_lo], axis=0).astype(BF)
        where = onehot(iota((LANES, rows), 0) == lane)
        coded = mm(coded, where, ((1,), (1,)))
        labels = coded[:owners] * 256.0 + coded[owners:]
        lives = jnp.broadcast_to(live_f, (SUB, rows)).astype(BF)
        counts = mm(lives, matches.astype(BF), ((1,), (1,)))[:1]
        half = hots // 2
        same = jnp.where(core == 0, counts[:, :half], counts[:, half:])
        flipped = jnp.where(core == 0, counts[:, half:], counts[:, :half])
        for p in range(owners):
            tags[p, :, :LANES] = labels[p : p + 1]
            tags[p, :, LANES:] = same if p % 2 == 0 else flipped
        tags_in[0, 0] = tags[0]

    def send_block(p):
        return remote(bucket.at[p - 1], arrived.at[0, p], send1, recv1.at[p], (partner(p), rep))

    def forward(q, p):
        return remote(
            arrived.at[0, p], arrived.at[q, p], send2, recv2.at[q, p], (me, other_rep(q))
        )

    def send_tag(p):
        return remote(tags.at[p], tags_in.at[0, p], tsend, trecv.at[p], (partner(p), rep))

    def pass_tags(q):
        return remote(tags_in.at[0], tags_in.at[q], tsend2, trecv2.at[q], (me, other_rep(q)))

    mate = (partner(1), rep)
    to_core = remote(hot_part.at[1 - core], hot_l1, hsend.at[0], h_core, mate)

    def to_near(d):
        there = partner(2 * d)
        index = lax.rem(there // 2, s.near)
        return remote(hot_s1.at[index], hot_l2.at[d], hsend.at[1], h_near.at[d], (there, rep))

    def to_rep(q):
        return remote(
            hot_s2.at[other_rep(q)], hot_l3.at[q], hsend.at[2], h_rep.at[q], (me, other_rep(q))
        )

    def to_far(f):
        return remote(
            hot_s3, hot_l4.at[f], hsend.at[3], h_far.at[f], (partner(2 * s.near * f), rep)
        )

    def to_all(d):
        return remote(
            hot_s4, hot_all.at[core, near], hsend.at[4], h_all.at[near], (partner(2 * d), rep)
        )

    def from_all(d):
        index = lax.rem(partner(2 * d) // 2, s.near)
        piece = hot_all.at[core, index]
        return pltpu.make_async_copy(piece, piece, h_all.at[index])

    to_mate = remote(hot_all.at[core], hot_all.at[core], hsend.at[5], h_last, mate)
    to_half = remote(half_ref, halves_ref.at[core], hsend.at[6], h_half, mate)

    def hot_start():
        hot_bf = (matches * live_f).astype(BF)
        sums = mm(hot_bf, feat_hi) + mm(hot_bf, feat_lo)
        hot_part[...] = sums.reshape(hot_part.shape)
        to_core.start()

    def hot_1():
        to_core.wait_recv()
        hot_s1[...] = hot_part[core] + hot_l1[...]
        for d in range(1, s.near):
            to_near(d).start()

    def hot_2():
        total = hot_s1[near]
        for d in range(1, s.near):
            to_near(d).wait_recv()
            total = total + hot_l2[d]
        hot_s2[...] = total
        for q in range(1, reps):
            to_rep(q).start()

    def hot_3():
        total = hot_s2[rep]
        for q in range(1, reps):
            to_rep(q).wait_recv()
            total = total + hot_l3[q]
        hot_s3[...] = total
        for f in range(1, s.far):
            to_far(f).start()

    def hot_4():
        total = hot_s3[...]
        for f in range(1, s.far):
            to_far(f).wait_recv()
            total = total + hot_l4[f]
        hot_s4[...] = total
        hot_all[core, near] = total
        for d in range(1, s.near):
            to_all(d).start()

    def hot_5():
        for d in range(1, s.near):
            from_all(d).wait()
        to_mate.start()

    def hot_6():
        to_half.wait_recv()
        mine = hots // reps
        j = iota((mine, LANES), 0)
        lane = (
            ((j & (s.part - 1)) >> log2(s.piece)) * (reps * s.piece)
            + rep * s.piece
            + (j & (s.piece - 1))
        )
        source = jnp.where(j < s.part, halves_ref[0], halves_ref[1])
        column = jnp.sum(
            jnp.where(iota((mine, LANES), 1) == lane, source, 0.0), axis=1, keepdims=True
        )
        hot_count_ref[...] = jnp.sum(
            jnp.where(iota((mine, mine), 0) == iota((mine, mine), 1), column, 0.0),
            axis=0,
            keepdims=True,
        )
        to_mate.wait_recv()
        everything = hot_all[...].reshape(mine, width)
        hot_sum_ref[...] = everything * (1.0 / jnp.sqrt(1.0 + column))

    base = rep * s.home_dev + 1

    def labels_of(q, g):
        lab = tags_in[q, g * s.pair, :, :LANES]
        for p in range(g * s.pair + 1, (g + 1) * s.pair):
            lab = lab + tags_in[q, p, :, :LANES]
        return lab.astype(jnp.int32) - base

    tiles = max(1, s.home_dev // 512)
    tile = s.home_dev // tiles

    def add(q, g, first=False, last=False):
        lab = labels_of(q, g)
        blocks = [arrived[q, g * s.pair + i] for i in range(s.pair)]
        hi, lo = split(jnp.concatenate(blocks, axis=0))
        both = jnp.concatenate([hi, lo], axis=0)
        for t in range(tiles):
            here = onehot(iota((tile, LANES), 0) + t * tile == lab)
            at = pl.ds(t * tile, tile)
            total = mm(jnp.concatenate([here, here], axis=1), both)
            if not first:
                total = sum_ref[at, :] + total
            if last:
                scale = scale_ref[at, :]
                total = total * jnp.concatenate([scale] * (width // LANES), axis=1)
            sum_ref[at, :] = total

    def pass_on(p):
        if p:
            send_block(p).wait_recv()
        for q in range(1, reps):
            forward(q, p).start()

    def tags_done():
        for p in range(1, owners):
            send_tag(p).wait_recv()
        for q in range(1, reps):
            pass_tags(q).start()

    def counts_done():
        for q in range(1, reps):
            pass_tags(q).wait_recv()
        total = jnp.sum(tags_in[...].reshape(reps * owners, width), axis=0, keepdims=True)
        half_ref[...] = total[:, LANES:]
        halves_ref[core] = total[:, LANES:]
        to_half.start()
        lab = jnp.concatenate(
            [labels_of(q, g) for q in range(reps) for g in range(s.pairs)], axis=1
        )
        n = lab.shape[1]
        up = max(SUB, s.home_rows)
        high = onehot(iota((up, n), 0) == (lab >> 7))
        low = onehot(iota((LANES, n), 0) == (lab & (LANES - 1)))
        count = mm(high, low, ((1,), (1,)))
        count_ref[...] = count[: s.home_rows]
        scale = 1.0 / jnp.sqrt(1.0 + count)
        for k in range(s.home_rows):
            wide = jnp.broadcast_to(scale[k : k + 1], (LANES, LANES))
            scale_ref[k * LANES : (k + 1) * LANES] = wide.T

    def peers(g, last=False):
        for q in range(1, reps):
            for p in range(g * s.pair, (g + 1) * s.pair):
                forward(q, p).wait_recv()
            add(q, g, last=last and q == reps - 1)

    chunks = owners // nb
    half = owners // 2
    held = range(owners - owners // 8, owners)
    make_tags()
    loads[4].wait()
    feat_hi, feat_lo = split(feat_ref[...])
    for c in range(chunks):
        place = onehot(iota((width, rows), 0) + c * width == slot)
        packed = mm(place, feat_hi) + mm(place, feat_lo)
        for i in range(nb):
            p = c * nb + i
            dst = arrived.at[0, 0] if p == 0 else bucket.at[p - 1]
            dst[...] = packed[i * cap : (i + 1) * cap]
        if c == 0:
            pl.semaphore_wait(barrier, owners + reps - 2)
        for p in range(c * nb, (c + 1) * nb):
            if p == 0:
                pass_on(0)
            elif p not in held:
                send_block(p).start()
        if c == 0:
            for p in range(1, owners):
                send_tag(p).start()
        if c == 1:
            hot_start()

    quarter = half // 2
    pairs = s.pairs
    for p in range(1, quarter):
        pass_on(p)
    hot_1()
    for p in range(quarter, half):
        pass_on(p)
    tags_done()
    for g in range(pairs // 4):
        add(0, g, first=g == 0)
    hot_2()
    for g in range(pairs // 4, pairs // 2):
        add(0, g)
    hot_3()
    for p in held:
        send_block(p).start()
    counts_done()
    peers(0)
    for g in range(pairs // 2, pairs):
        for p in range(g * s.pair, (g + 1) * s.pair):
            pass_on(p)
        if g == pairs // 2:
            hot_4()
        if g == pairs - 2:
            hot_5()
        if g > pairs // 2:
            add(0, g - 1)
            peers(g - pairs // 2)
    add(0, pairs - 1)
    hot_6()
    for g in range(pairs // 2, pairs):
        peers(g, last=g == pairs - 1)

    to_core.wait_send()
    for d in range(1, s.near):
        to_near(d).wait_send()
        to_all(d).wait_send()
    for q in range(1, reps):
        to_rep(q).wait_send()
        pass_tags(q).wait_send()
    for f in range(1, s.far):
        to_far(f).wait_send()
    to_mate.wait_send()
    to_half.wait_send()
    sent = tags.at[pl.ds(1, owners - 1)]
    pltpu.make_async_copy(sent, sent, tsend).wait()
    pltpu.make_async_copy(bucket, bucket, send1).wait()
    if reps > 1:
        sent = arrived.at[pl.ds(1, reps - 1)]
        pltpu.make_async_copy(sent, sent, send2).wait()


def local(features, group_ids, survive, home_row, hot_ids):
    rows, width = features.shape
    groups, hots = home_row.shape[0], hot_ids.shape[0]
    s = Sizes(lax.axis_size("owner"), lax.axis_size("rep"), rows, width, groups, hots)
    owners, reps = s.owners, s.reps
    vmem = pl.BlockSpec(memory_space=pltpu.VMEM)
    hbm = pl.BlockSpec(memory_space=pltpu.HBM)
    DMA = pltpu.SemaphoreType.DMA
    VM = pltpu.VMEM
    operands = (
        group_ids.reshape(1, rows),
        survive.reshape(1, rows),
        hot_ids.reshape(1, hots),
        home_row.reshape(groups // LANES, LANES),
        features,
    )
    operands = [pltpu.with_memory_space_constraint(x, pltpu.HBM) for x in operands]
    cold_sum, count, hot_sum, hot_count = pl.pallas_call(
        functools.partial(kernel, s),
        out_shape=(
            pltpu.VMEM((s.home_dev, width), F32),
            pltpu.VMEM((s.home_rows, LANES), F32),
            pltpu.VMEM((hots // reps, width), F32),
            pltpu.VMEM((1, hots // reps), F32),
        ),
        in_specs=[hbm] * 5,
        out_specs=[vmem] * 4,
        scratch_shapes=[
            VM((1, rows), jnp.int32),
            VM((1, rows), jnp.int32),
            VM((1, hots), jnp.int32),
            VM((groups // LANES, LANES), jnp.int32),
            VM((rows, width), F32),
            VM((owners - 1, s.cap, width), F32),
            VM((reps, owners, s.cap, width), F32),
            VM((owners, 1, width), F32),
            VM((reps, owners, 1, width), F32),
            VM((s.home_dev, LANES), F32),
            VM((2, s.near, reps, s.piece, width), F32),
            VM((s.near, reps, s.piece, width), F32),
            VM((s.near, reps, s.piece, width), F32),
            VM((s.near, reps, s.piece, width), F32),
            VM((reps, s.piece, width), F32),
            VM((reps, s.piece, width), F32),
            VM((s.piece, width), F32),
            VM((s.far, s.piece, width), F32),
            VM((s.piece, width), F32),
            VM((2, s.near, s.piece, width), F32),
            VM((1, LANES), F32),
            VM((2, 1, LANES), F32),
            DMA((5,)),
            DMA(()),
            DMA((owners,)),
            DMA(()),
            DMA((reps, owners)),
            DMA(()),
            DMA((owners,)),
            DMA(()),
            DMA((reps,)),
            DMA((7,)),
            DMA(()),
            DMA((s.near,)),
            DMA((reps,)),
            DMA((s.far,)),
            DMA((s.near,)),
            DMA(()),
            DMA(()),
        ],
        compiler_params=pltpu.CompilerParams(
            collective_id=0, has_side_effects=True, vmem_limit_bytes=48 << 20
        ),
    )(*operands)
    return cold_sum, count.reshape(s.home_dev), hot_sum, hot_count.reshape(hots // reps)


def solution(mesh):
    in_specs = (P(("owner", "rep"), None), P(("owner", "rep")), P(("owner", "rep")), P(), P())
    out_specs = (P(("owner", "rep"), None), P(("owner", "rep")), P("rep", None), P("rep"))
    return jax.shard_map(local, mesh=mesh, in_specs=in_specs, out_specs=out_specs, check_vma=False)
```

```python
import functools

import jax
import jax.numpy as jnp
from jax import lax
from jax.experimental import pallas as pl
from jax.experimental.pallas import tpu as pltpu
from jax.sharding import PartitionSpec as P

MESH = pl.DeviceIdType.MESH
LANES = 128
SUB = 8
BF = jnp.bfloat16
F32 = jnp.float32


def iota(shape, axis):
    return lax.broadcasted_iota(jnp.int32, shape, axis)


def mm(a, b, dims=((1,), (0,))):
    return lax.dot_general(a, b, (dims, ((), ())), preferred_element_type=F32)


def split(x):
    hi = x.astype(BF)
    return hi, (x - hi.astype(F32)).astype(BF)


def onehot(mask):
    return jnp.where(mask, 1.0, 0.0).astype(BF)


def log2(n):
    return n.bit_length() - 1


PLAN = (
    "M0", "K0", "B0", "s1", "s2", "s3", "f0", "t0", "K1", "s4", "H0", "s5",
    "s6", "s7", "K2", "s8", "s9", "K3", "s10", "s11", "f1", "f2", "f3", "H1",
    "s12", "s13", "f4", "f5", "f6", "f7", "T0", "a0", "a1", "a2", "H2", "f11",
    "a3", "f9", "H3", "s14", "s15", "f10", "f8", "a4", "f12", "f13", "p2", "H4",
    "p0", "f14", "f15", "a7", "a6", "p1", "p3", "a5", "H5", "p4", "p5", "p6",
    "C0", "H6", "p7",
)


class Sizes:
    def __init__(self, owners, reps, rows, width, groups, hots):
        self.owners, self.reps, self.rows, self.width, self.hots = owners, reps, rows, width, hots
        self.groups = groups
        self.own_groups = groups // owners
        self.home_dev = self.own_groups // reps
        self.cap = 2 * rows // owners
        self.nb = width // self.cap
        self.pair = LANES // self.cap
        self.pairs = owners // self.pair
        self.chips = owners // 2
        self.part = hots // reps // 2
        self.near = min(self.chips // 2, self.part // SUB)
        self.far = self.chips // self.near
        self.piece = self.part // self.near
        self.home_rows = self.home_dev // LANES
        self.parts = width // LANES
        self.block = self.parts * self.cap + 1
        self.hot_block = self.parts * self.piece + 1
        self.count_rows = max(SUB, self.home_rows)


def kernel(
    s,
    ids_hbm,
    survive_hbm,
    hot_hbm,
    table_hbm,
    feat_hbm,
    sum_ref,
    count_ref,
    hot_sum_ref,
    hot_count_ref,
    ids_ref,
    survive_ref,
    hot_ref,
    table_ref,
    feat_ref,
    bucket,
    arrived,
    tags,
    tags_in,
    tally_ref,
    scale_ref,
    hot_part,
    hot_l1,
    hot_s1,
    hot_l2,
    hot_s2,
    hot_l3,
    hot_s3,
    hot_l4,
    hot_s4,
    hot_all,
    load,
    send1,
    recv1,
    send2,
    recv2,
    tsend,
    trecv,
    tsend2,
    trecv2,
    hsend,
    h_core,
    h_near,
    h_rep,
    h_far,
    h_all,
    h_last,
):
    owners, reps, cap, nb = s.owners, s.reps, s.cap, s.nb
    rows, width, hots = s.rows, s.width, s.hots
    me = lax.axis_index("owner")
    rep = lax.axis_index("rep")
    core = lax.rem(me, 2)
    near = lax.rem(me // 2, s.near)

    loads = [
        pltpu.make_async_copy(src, dst, load.at[i])
        for i, (src, dst) in enumerate(
            (
                (table_hbm, table_ref),
                (ids_hbm, ids_ref),
                (survive_hbm, survive_ref),
                (hot_hbm, hot_ref),
                (feat_hbm, feat_ref),
            )
        )
    ]
    for copy in loads:
        copy.start()

    barrier = pltpu.get_barrier_semaphore()

    @pl.loop(1, owners)
    def _(d):
        pl.semaphore_signal(
            barrier, inc=1, device_id=(lax.rem(me + d, owners), rep), device_id_type=MESH
        )

    @pl.loop(1, reps)
    def _(d):
        pl.semaphore_signal(
            barrier, inc=1, device_id=(me, lax.rem(rep + d, reps)), device_id_type=MESH
        )

    flips = []
    bit = 1
    while bit < owners:
        flips.append((bit, bit - 2 * bit * lax.rem(me // bit, 2)))
        bit *= 2

    def partner(p):
        out = me
        for bit, flip in flips:
            if p & bit:
                out = out + flip
        return out

    def other_rep(q):
        return lax.rem(rep + q, reps)

    def remote(src, dst, send, recv, device):
        return pltpu.make_async_remote_copy(
            src_ref=src,
            dst_ref=dst,
            send_sem=send,
            recv_sem=recv,
            device_id=device,
            device_id_type=MESH,
        )

    for copy in loads[:4]:
        copy.wait()
    ids = ids_ref[...]
    live_f = jnp.where(survive_ref[...] == 1, 1.0, 0.0)
    table = table_ref[...]
    trows = table.shape[0]
    halves = jnp.concatenate([table >> 8, table & 255], axis=1).astype(F32).astype(BF)
    pick = onehot(iota((trows, rows), 0) == (ids >> 7))
    both = mm(halves, pick, ((0,), (0,)))
    column = both[:LANES] * 256.0 + both[LANES:]
    home = jnp.sum(
        jnp.where(iota((LANES, rows), 0) == (ids & (LANES - 1)), column, 0.0), axis=0, keepdims=True
    )
    target = jnp.floor(home * (1.0 / s.own_groups))
    label = home - target * s.own_groups + 1.0
    place_at = target.astype(jnp.int32) ^ me

    at = iota((hots, hots), 0)
    block = at >> log2(s.piece)
    number = (
        (block & (reps - 1)) * (2 * s.part)
        + (block >> log2(reps)) * s.piece
        + (at & (s.piece - 1))
    )
    hot_col = jnp.sum(
        jnp.where(number == iota((hots, hots), 1), hot_ref[...].astype(F32), 0.0),
        axis=1,
        keepdims=True,
    )
    matches = jnp.where(hot_col == ids.astype(F32), 1.0, 0.0)
    is_hot = jnp.max(matches, axis=0, keepdims=True)
    keep = live_f * (1.0 - is_hot)
    place_at = jnp.where(keep > 0.0, place_at, -1)

    member = jnp.where(iota((owners, rows), 0) == place_at, 1.0, 0.0)
    before = onehot(iota((rows, rows), 0) < iota((rows, rows), 1))
    position = mm(member.astype(BF), before)
    placed = jnp.sum(position * member, axis=0, keepdims=True).astype(jnp.int32)
    slot = jnp.where(keep > 0.0, place_at * cap + placed, -1)

    last_pair = owners - s.pair

    def make_tags():
        lane = placed + cap * (place_at & (s.pair - 1))
        label_hi = jnp.floor(label * (1.0 / 256.0))
        label_lo = label - 256.0 * label_hi
        coded = jnp.concatenate([member * label_hi, member * label_lo], axis=0).astype(BF)
        where = onehot(iota((LANES, rows), 0) == lane)
        coded = mm(coded, where, ((1,), (1,)))
        labels = coded[:owners] * 256.0 + coded[owners:]
        for p in range(owners):
            block_of(p)[s.block - 1 :] = labels[p : p + 1]
        for p in range(last_pair, owners):
            tags[p - last_pair] = labels[p : p + 1]

    def block_of(p):
        return arrived.at[0, 0] if p == 0 else bucket.at[p - 1]

    def unfold(ref, n):
        return jnp.concatenate([ref[k * n : (k + 1) * n] for k in range(s.parts)], axis=1)

    def send_block(p):
        return remote(bucket.at[p - 1], arrived.at[0, p], send1, recv1.at[p], (partner(p), rep))

    def forward(q, p):
        return remote(
            arrived.at[0, p], arrived.at[q, p], send2, recv2.at[q, p], (me, other_rep(q))
        )

    def send_tag(p):
        i = p - last_pair
        return remote(tags.at[i], tags_in.at[0, i], tsend, trecv.at[i], (partner(p), rep))

    def pass_tags(q):
        return remote(tags_in.at[0], tags_in.at[q], tsend2, trecv2.at[q], (me, other_rep(q)))

    mate = (partner(1), rep)
    to_core = remote(hot_part.at[1 - core], hot_l1, hsend.at[0], h_core, mate)

    def to_near(d):
        there = partner(2 * d)
        index = lax.rem(there // 2, s.near)
        return remote(hot_s1.at[index], hot_l2.at[d], hsend.at[1], h_near.at[d], (there, rep))

    def to_rep(q):
        return remote(
            hot_s2.at[other_rep(q)], hot_l3.at[q], hsend.at[2], h_rep.at[q], (me, other_rep(q))
        )

    def to_far(f):
        return remote(
            hot_s3, hot_l4.at[f], hsend.at[3], h_far.at[f], (partner(2 * s.near * f), rep)
        )

    def to_all(d):
        return remote(
            hot_s4, hot_all.at[core, near], hsend.at[4], h_all.at[near], (partner(2 * d), rep)
        )

    def from_all(d):
        index = lax.rem(partner(2 * d) // 2, s.near)
        piece = hot_all.at[core, index]
        return pltpu.make_async_copy(piece, piece, h_all.at[index])

    to_mate = remote(hot_all.at[core], hot_all.at[core], hsend.at[5], h_last, mate)

    def hot_start():
        hot_bf = (matches * live_f).astype(BF)
        sums = mm(hot_bf, feats[0]) + mm(hot_bf, feats[1])
        lives = jnp.broadcast_to(live_f, (SUB, rows)).astype(BF)
        counts = mm(lives, hot_bf, ((1,), (1,)))[:1]
        shape = (2, s.near, reps, s.piece, LANES)
        for k in range(s.parts):
            part = sums[:, k * LANES : (k + 1) * LANES].reshape(shape)
            hot_part[:, :, :, k * s.piece : (k + 1) * s.piece] = part
        half = hots // 2
        for c in range(2):
            for n in range(s.near):
                for r in range(reps):
                    hot_part[c, n, r, s.hot_block - 1 :] = counts[:, c * half : (c + 1) * half]
        to_core.start()

    def hot_1():
        to_core.wait_recv()
        hot_s1[...] = hot_part[core] + hot_l1[...]
        for d in range(1, s.near):
            to_near(d).start()

    def hot_2():
        total = hot_s1[near]
        for d in range(1, s.near):
            to_near(d).wait_recv()
            total = total + hot_l2[d]
        hot_s2[...] = total
        for q in range(1, reps):
            to_rep(q).start()

    def hot_3():
        total = hot_s2[rep]
        for q in range(1, reps):
            to_rep(q).wait_recv()
            total = total + hot_l3[q]
        hot_s3[...] = total
        for f in range(1, s.far):
            to_far(f).start()

    def hot_4():
        total = hot_s3[...]
        for f in range(1, s.far):
            to_far(f).wait_recv()
            total = total + hot_l4[f]
        hot_s4[...] = total
        hot_all[core, near] = total
        for d in range(1, s.near):
            to_all(d).start()

    def hot_5():
        for d in range(1, s.near):
            from_all(d).wait()
        to_mate.start()

    def hot_6():
        to_mate.wait_recv()
        mine = hots // reps
        order = [(c, n) for c in range(2) for n in range(s.near)]
        source = jnp.concatenate(
            [
                jnp.broadcast_to(hot_all[c, n, s.hot_block - 1 :], (s.piece, LANES))
                for c, n in order
            ],
            axis=0,
        )
        j = iota((mine, LANES), 0)
        lane = (
            ((j & (s.part - 1)) >> log2(s.piece)) * (reps * s.piece)
            + rep * s.piece
            + (j & (s.piece - 1))
        )
        column = jnp.sum(
            jnp.where(iota((mine, LANES), 1) == lane, source, 0.0), axis=1, keepdims=True
        )
        hot_count_ref[...] = jnp.sum(
            jnp.where(iota((mine, mine), 0) == iota((mine, mine), 1), column, 0.0),
            axis=0,
            keepdims=True,
        )
        everything = jnp.concatenate(
            [unfold(hot_all.at[c, n], s.piece) for c, n in order], axis=0
        )
        hot_sum_ref[...] = everything * (1.0 / jnp.sqrt(1.0 + column))

    base = rep * s.home_dev + 1

    def place_of(rows_of):
        return functools.reduce(jnp.add, rows_of).astype(jnp.int32) - base

    def tally(lab):
        high = onehot(iota((s.count_rows, LANES), 0) == (lab >> 7))
        low = onehot(iota((LANES, LANES), 0) == (lab & (LANES - 1)))
        return mm(high, low, ((1,), (1,)))

    tiles = max(1, s.home_dev // 512)
    tile = s.home_dev // tiles

    def add(q, g, first=False, last=False):
        own = range(g * s.pair, (g + 1) * s.pair)
        lab = place_of([arrived[q, p, s.block - 1 :] for p in own])
        if first:
            tally_ref[...] = tally(lab)
        elif g < s.pairs - 1:
            tally_ref[...] += tally(lab)
        blocks = [unfold(arrived.at[q, p], cap) for p in own]
        hi, lo = split(jnp.concatenate(blocks, axis=0))
        both = jnp.concatenate([hi, lo], axis=0)
        for t in range(tiles):
            here = onehot(iota((tile, LANES), 0) + t * tile == lab)
            at = pl.ds(t * tile, tile)
            total = mm(jnp.concatenate([here, here], axis=1), both)
            if not first:
                total = sum_ref[at, :] + total
            if last:
                scale = scale_ref[at, :]
                total = total * jnp.concatenate([scale] * (width // LANES), axis=1)
            sum_ref[at, :] = total

    def pass_on(p):
        if p:
            send_block(p).wait_recv()
        for q in range(1, reps):
            forward(q, p).start()

    def tags_done():
        for p in range(last_pair, owners):
            send_tag(p).wait_recv()
        for q in range(1, reps):
            pass_tags(q).start()

    def counts_done():
        count = tally_ref[...]
        for q in range(reps):
            if q:
                pass_tags(q).wait_recv()
            count = count + tally(place_of([tags_in[q, i] for i in range(s.pair)]))
        count_ref[...] = count[: s.home_rows]
        scale = 1.0 / jnp.sqrt(1.0 + count)
        for k in range(s.home_rows):
            wide = jnp.broadcast_to(scale[k : k + 1], (LANES, LANES))
            scale_ref[k * LANES : (k + 1) * LANES] = wide.T

    def peers(g, last=False):
        for q in range(1, reps):
            for p in range(g * s.pair, (g + 1) * s.pair):
                forward(q, p).wait_recv()
            add(q, g, last=last and q == reps - 1)

    unit = s.pair // 2
    feats = []

    def pack(c):
        if c == 0:
            loads[4].wait()
            feats.extend(split(feat_ref[...]))
        place = onehot(iota((width, rows), 0) + c * width == slot)
        packed = mm(place, feats[0]) + mm(place, feats[1])
        for i in range(nb):
            p = c * nb + i
            for k in range(s.parts):
                part = packed[i * cap : (i + 1) * cap, k * LANES : (k + 1) * LANES]
                block_of(p)[k * cap : (k + 1) * cap] = part

    def send(u):
        for p in range(max(1, u * unit), (u + 1) * unit):
            send_block(p).start()

    def follow(u):
        for p in range(u * unit, (u + 1) * unit):
            pass_on(p)

    def send_tags():
        for p in range(last_pair, owners):
            send_tag(p).start()

    def enter():
        pl.semaphore_wait(barrier, owners + reps - 2)

    steps = {
        "M": lambda n: make_tags(),
        "K": pack,
        "B": lambda n: enter(),
        "s": send,
        "f": follow,
        "t": lambda n: send_tags(),
        "T": lambda n: tags_done(),
        "C": lambda n: counts_done(),
        "a": lambda n: add(0, n, first=n == 0),
        "p": lambda n: peers(n, last=n == s.pairs - 1),
        "H": lambda n: (hot_start, hot_1, hot_2, hot_3, hot_4, hot_5, hot_6)[n](),
    }
    for step in PLAN:
        steps[step[0]](int(step[1:]))

    to_core.wait_send()
    for d in range(1, s.near):
        to_near(d).wait_send()
        to_all(d).wait_send()
    for q in range(1, reps):
        to_rep(q).wait_send()
        pass_tags(q).wait_send()
    for f in range(1, s.far):
        to_far(f).wait_send()
    to_mate.wait_send()
    pltpu.make_async_copy(tags, tags, tsend).wait()
    pltpu.make_async_copy(bucket, bucket, send1).wait()
    if reps > 1:
        sent = arrived.at[pl.ds(1, reps - 1)]
        pltpu.make_async_copy(sent, sent, send2).wait()


def write_out(*refs):
    n = len(refs) // 2
    sems = refs[-1]
    copies = [pltpu.make_async_copy(refs[i], refs[n + i], sems.at[i]) for i in range(n)]
    for copy in copies:
        copy.start()
    for copy in copies:
        copy.wait()


def local(features, group_ids, survive, home_row, hot_ids):
    rows, width = features.shape
    groups, hots = home_row.shape[0], hot_ids.shape[0]
    s = Sizes(lax.axis_size("owner"), lax.axis_size("rep"), rows, width, groups, hots)
    owners, reps = s.owners, s.reps
    vmem = pl.BlockSpec(memory_space=pltpu.VMEM)
    hbm = pl.BlockSpec(memory_space=pltpu.HBM)
    DMA = pltpu.SemaphoreType.DMA
    VM = pltpu.VMEM
    operands = (
        group_ids.reshape(1, rows),
        survive.reshape(1, rows),
        hot_ids.reshape(1, hots),
        home_row.reshape(groups // LANES, LANES),
        features,
    )
    operands = [pltpu.with_memory_space_constraint(x, pltpu.HBM) for x in operands]
    results = pl.pallas_call(
        functools.partial(kernel, s),
        out_shape=(
            pltpu.VMEM((s.home_dev, width), F32),
            pltpu.VMEM((s.home_rows, LANES), F32),
            pltpu.VMEM((hots // reps, width), F32),
            pltpu.VMEM((1, hots // reps), F32),
        ),
        in_specs=[hbm] * 5,
        out_specs=[vmem] * 4,
        scratch_shapes=[
            VM((1, rows), jnp.int32),
            VM((1, rows), jnp.int32),
            VM((1, hots), jnp.int32),
            VM((groups // LANES, LANES), jnp.int32),
            VM((rows, width), F32),
            VM((owners - 1, s.block, LANES), F32),
            VM((reps, owners, s.block, LANES), F32),
            VM((s.pair, 1, LANES), F32),
            VM((reps, s.pair, 1, LANES), F32),
            VM((s.count_rows, LANES), F32),
            VM((s.home_dev, LANES), F32),
            VM((2, s.near, reps, s.hot_block, LANES), F32),
            VM((s.near, reps, s.hot_block, LANES), F32),
            VM((s.near, reps, s.hot_block, LANES), F32),
            VM((s.near, reps, s.hot_block, LANES), F32),
            VM((reps, s.hot_block, LANES), F32),
            VM((reps, s.hot_block, LANES), F32),
            VM((s.hot_block, LANES), F32),
            VM((s.far, s.hot_block, LANES), F32),
            VM((s.hot_block, LANES), F32),
            VM((2, s.near, s.hot_block, LANES), F32),
            DMA((5,)),
            DMA(()),
            DMA((owners,)),
            DMA(()),
            DMA((reps, owners)),
            DMA(()),
            DMA((s.pair,)),
            DMA(()),
            DMA((reps,)),
            DMA((6,)),
            DMA(()),
            DMA((s.near,)),
            DMA((reps,)),
            DMA((s.far,)),
            DMA((s.near,)),
            DMA(()),
        ],
        compiler_params=pltpu.CompilerParams(
            collective_id=0, has_side_effects=True, vmem_limit_bytes=48 << 20
        ),
    )(*operands)
    results = [pltpu.with_memory_space_constraint(x, pltpu.VMEM) for x in results]
    cold_sum, count, hot_sum, hot_count = pl.pallas_call(
        write_out,
        out_shape=[jax.ShapeDtypeStruct(x.shape, x.dtype) for x in results],
        in_specs=[vmem] * 4,
        out_specs=[hbm] * 4,
        scratch_shapes=[DMA((4,))],
    )(*results)
    return cold_sum, count.reshape(s.home_dev), hot_sum, hot_count.reshape(hots // reps)


def solution(mesh):
    in_specs = (P(("owner", "rep"), None), P(("owner", "rep")), P(("owner", "rep")), P(), P())
    out_specs = (P(("owner", "rep"), None), P(("owner", "rep")), P("rep", None), P("rep"))
    return jax.shard_map(local, mesh=mesh, in_specs=in_specs, out_specs=out_specs, check_vma=False)
```

```python
import functools

import jax
import jax.numpy as jnp
from jax import lax
from jax.experimental import pallas as pl
from jax.experimental.pallas import tpu as pltpu
from jax.sharding import PartitionSpec as P

MESH = pl.DeviceIdType.MESH
LANES = 128
SUB = 8
BF = jnp.bfloat16
F32 = jnp.float32


def iota(shape, axis):
    return lax.broadcasted_iota(jnp.int32, shape, axis)


def mm(a, b, dims=((1,), (0,))):
    return lax.dot_general(a, b, (dims, ((), ())), preferred_element_type=F32)


def split(x):
    hi = x.astype(BF)
    return hi, (x - hi.astype(F32)).astype(BF)


def onehot(mask):
    return jnp.where(mask, 1.0, 0.0).astype(BF)


def log2(n):
    return n.bit_length() - 1


PLAN = (
    "M0", "K0", "B0", "s1", "s3", "s2", "f0", "t0", "K1", "s4", "H0", "s5",
    "s6", "s7", "K2", "s8", "s9", "s10", "K3", "f1", "H1", "s11", "s13", "f2",
    "f3", "f4", "f5", "f6", "s12", "f7", "T0", "a0", "a1", "H2", "f8", "f9",
    "H3", "s14", "s15", "f10", "f11", "a2", "a3", "p0", "f12", "a4", "f13", "H4",
    "p1", "f14", "f15", "a5", "a6", "a7", "p2", "p4", "p3", "H5", "p5", "p6",
    "C0", "H6", "p7",
)

ORDERS = (
    (0, 1, 3, 2, 4, 5, 9, 6, 7, 8, 10, 11, 12, 13, 14, 15),
    (0, 1, 2, 8, 3, 9, 10, 11, 4, 5, 6, 7, 12, 13, 15, 14),
    (0, 1, 2, 8, 3, 10, 4, 9, 5, 6, 7, 12, 13, 11, 14, 15),
)


class Sizes:
    def __init__(self, owners, reps, rows, width, groups, hots):
        self.owners, self.reps, self.rows, self.width, self.hots = owners, reps, rows, width, hots
        self.groups = groups
        self.own_groups = groups // owners
        self.home_dev = self.own_groups // reps
        self.cap = 2 * rows // owners
        self.nb = width // self.cap
        self.pair = LANES // self.cap
        self.pairs = owners // self.pair
        self.chips = owners // 2
        self.part = hots // reps // 2
        self.near = min(self.chips // 2, self.part // SUB)
        self.far = self.chips // self.near
        self.piece = self.part // self.near
        self.home_rows = self.home_dev // LANES
        self.parts = width // LANES
        self.block = self.parts * self.cap + 1
        self.hot_block = self.parts * self.piece + 1
        self.count_rows = max(SUB, self.home_rows)


def kernel(
    s,
    ids_hbm,
    survive_hbm,
    hot_hbm,
    table_hbm,
    feat_hbm,
    sum_ref,
    count_ref,
    hot_sum_ref,
    hot_count_ref,
    ids_ref,
    survive_ref,
    hot_ref,
    table_ref,
    feat_ref,
    bucket,
    arrived,
    tags,
    tags_in,
    tally_ref,
    scale_ref,
    hot_part,
    hot_l1,
    hot_s1,
    hot_l2,
    hot_s2,
    hot_l3,
    hot_s3,
    hot_l4,
    hot_s4,
    hot_all,
    load,
    send1,
    recv1,
    send2,
    recv2,
    tsend,
    trecv,
    tsend2,
    trecv2,
    hsend,
    h_core,
    h_near,
    h_rep,
    h_far,
    h_all,
    h_last,
):
    owners, reps, cap, nb = s.owners, s.reps, s.cap, s.nb
    unit = s.pair // 2
    rows, width, hots = s.rows, s.width, s.hots
    me = lax.axis_index("owner")
    rep = lax.axis_index("rep")
    core = lax.rem(me, 2)
    near = lax.rem(me // 2, s.near)

    loads = [
        pltpu.make_async_copy(src, dst, load.at[i])
        for i, (src, dst) in enumerate(
            (
                (table_hbm, table_ref),
                (ids_hbm, ids_ref),
                (survive_hbm, survive_ref),
                (hot_hbm, hot_ref),
                (feat_hbm, feat_ref),
            )
        )
    ]
    for copy in loads:
        copy.start()

    barrier = pltpu.get_barrier_semaphore()

    @pl.loop(1, owners)
    def _(d):
        pl.semaphore_signal(
            barrier, inc=1, device_id=(lax.rem(me + d, owners), rep), device_id_type=MESH
        )

    @pl.loop(1, reps)
    def _(d):
        pl.semaphore_signal(
            barrier, inc=1, device_id=(me, lax.rem(rep + d, reps)), device_id_type=MESH
        )

    flips = []
    bit = 1
    while bit < owners:
        flips.append((bit, bit - 2 * bit * lax.rem(me // bit, 2)))
        bit *= 2

    def partner(p):
        out = me
        for bit, flip in flips:
            if p & bit:
                out = out + flip
        return out

    def other_rep(q):
        return lax.rem(rep + q, reps)

    def remote(src, dst, send, recv, device):
        return pltpu.make_async_remote_copy(
            src_ref=src,
            dst_ref=dst,
            send_sem=send,
            recv_sem=recv,
            device_id=device,
            device_id_type=MESH,
        )

    for copy in loads[:4]:
        copy.wait()
    ids = ids_ref[...]
    live_f = jnp.where(survive_ref[...] == 1, 1.0, 0.0)
    table = table_ref[...]
    trows = table.shape[0]
    halves = jnp.concatenate([table >> 8, table & 255], axis=1).astype(F32).astype(BF)
    pick = onehot(iota((trows, rows), 0) == (ids >> 7))
    both = mm(halves, pick, ((0,), (0,)))
    column = both[:LANES] * 256.0 + both[LANES:]
    home = jnp.sum(
        jnp.where(iota((LANES, rows), 0) == (ids & (LANES - 1)), column, 0.0), axis=0, keepdims=True
    )
    target = jnp.floor(home * (1.0 / s.own_groups))
    label = home - target * s.own_groups + 1.0
    place_at = target.astype(jnp.int32) ^ me

    at = iota((hots, hots), 0)
    block = at >> log2(s.piece)
    number = (
        (block & (reps - 1)) * (2 * s.part)
        + (block >> log2(reps)) * s.piece
        + (at & (s.piece - 1))
    )
    hot_col = jnp.sum(
        jnp.where(number == iota((hots, hots), 1), hot_ref[...].astype(F32), 0.0),
        axis=1,
        keepdims=True,
    )
    matches = jnp.where(hot_col == ids.astype(F32), 1.0, 0.0)
    is_hot = jnp.max(matches, axis=0, keepdims=True)
    keep = live_f * (1.0 - is_hot)
    place_at = jnp.where(keep > 0.0, place_at, -1)

    member = jnp.where(iota((owners, rows), 0) == place_at, 1.0, 0.0)
    before = onehot(iota((rows, rows), 0) < iota((rows, rows), 1))
    position = mm(member.astype(BF), before)
    placed = jnp.sum(position * member, axis=0, keepdims=True).astype(jnp.int32)
    slot = jnp.where(keep > 0.0, place_at * cap + placed, -1)

    last_pair = owners - s.pair

    def make_tags():
        lane = placed + cap * (place_at & (s.pair - 1))
        label_hi = jnp.floor(label * (1.0 / 256.0))
        label_lo = label - 256.0 * label_hi
        coded = jnp.concatenate([member * label_hi, member * label_lo], axis=0).astype(BF)
        where = onehot(iota((LANES, rows), 0) == lane)
        coded = mm(coded, where, ((1,), (1,)))
        labels = coded[:owners] * 256.0 + coded[owners:]
        for p in range(owners):
            block_of(p)[s.block - 1 :] = labels[p : p + 1]
        for p in range(last_pair, owners):
            tags[p - last_pair] = labels[p : p + 1]

    def block_of(p):
        return arrived.at[0, 0] if p == 0 else bucket.at[p - 1]

    def unfold(ref, n):
        return jnp.concatenate([ref[k * n : (k + 1) * n] for k in range(s.parts)], axis=1)

    spans = (pl.ds(0, s.block),)

    def send_block(p):
        for i, span in enumerate(spans):
            remote(
                bucket.at[p - 1, span],
                arrived.at[0, p, span],
                send1,
                recv1.at[p, i],
                (partner(p), rep),
            ).start()

    def forward(q, p, i):
        piece = arrived.at[0, p, spans[i]]
        return remote(
            piece, arrived.at[q, p, spans[i]], send2, recv2.at[q, p, i], (me, other_rep(q))
        )

    def send_tag(p):
        i = p - last_pair
        return remote(tags.at[i], tags_in.at[0, i], tsend, trecv.at[i], (partner(p), rep))

    def pass_tags(q):
        return remote(tags_in.at[0], tags_in.at[q], tsend2, trecv2.at[q], (me, other_rep(q)))

    mate = (partner(1), rep)
    to_core = remote(hot_part.at[1 - core], hot_l1, hsend.at[0], h_core, mate)

    def to_near(d):
        there = partner(2 * d)
        index = lax.rem(there // 2, s.near)
        return remote(hot_s1.at[index], hot_l2.at[d], hsend.at[1], h_near.at[d], (there, rep))

    def to_rep(q):
        return remote(
            hot_s2.at[other_rep(q)], hot_l3.at[q], hsend.at[2], h_rep.at[q], (me, other_rep(q))
        )

    def to_far(f):
        return remote(
            hot_s3, hot_l4.at[f], hsend.at[3], h_far.at[f], (partner(2 * s.near * f), rep)
        )

    def to_all(d):
        return remote(
            hot_s4, hot_all.at[core, near], hsend.at[4], h_all.at[near], (partner(2 * d), rep)
        )

    def from_all(d):
        index = lax.rem(partner(2 * d) // 2, s.near)
        piece = hot_all.at[core, index]
        return pltpu.make_async_copy(piece, piece, h_all.at[index])

    to_mate = remote(hot_all.at[core], hot_all.at[core], hsend.at[5], h_last, mate)

    def hot_start():
        hot_bf = (matches * live_f).astype(BF)
        sums = mm(hot_bf, feats[0]) + mm(hot_bf, feats[1])
        lives = jnp.broadcast_to(live_f, (SUB, rows)).astype(BF)
        counts = mm(lives, hot_bf, ((1,), (1,)))[:1]
        shape = (2, s.near, reps, s.piece, LANES)
        for k in range(s.parts):
            part = sums[:, k * LANES : (k + 1) * LANES].reshape(shape)
            hot_part[:, :, :, k * s.piece : (k + 1) * s.piece] = part
        half = hots // 2
        for c in range(2):
            for n in range(s.near):
                for r in range(reps):
                    hot_part[c, n, r, s.hot_block - 1 :] = counts[:, c * half : (c + 1) * half]
        to_core.start()

    def hot_1():
        to_core.wait_recv()
        hot_s1[...] = hot_part[core] + hot_l1[...]
        for d in range(1, s.near):
            to_near(d).start()

    def hot_2():
        total = hot_s1[near]
        for d in range(1, s.near):
            to_near(d).wait_recv()
            total = total + hot_l2[d]
        hot_s2[...] = total
        for q in range(1, reps):
            to_rep(q).start()

    def hot_3():
        total = hot_s2[rep]
        for q in range(1, reps):
            to_rep(q).wait_recv()
            total = total + hot_l3[q]
        hot_s3[...] = total
        for f in range(1, s.far):
            to_far(f).start()

    def hot_4():
        total = hot_s3[...]
        for f in range(1, s.far):
            to_far(f).wait_recv()
            total = total + hot_l4[f]
        hot_s4[...] = total
        hot_all[core, near] = total
        for d in range(1, s.near):
            to_all(d).start()

    def hot_5():
        for d in range(1, s.near):
            from_all(d).wait()
        to_mate.start()

    def hot_6():
        to_mate.wait_recv()
        mine = hots // reps
        order = [(c, n) for c in range(2) for n in range(s.near)]
        source = jnp.concatenate(
            [
                jnp.broadcast_to(hot_all[c, n, s.hot_block - 1 :], (s.piece, LANES))
                for c, n in order
            ],
            axis=0,
        )
        j = iota((mine, LANES), 0)
        lane = (
            ((j & (s.part - 1)) >> log2(s.piece)) * (reps * s.piece)
            + rep * s.piece
            + (j & (s.piece - 1))
        )
        column = jnp.sum(
            jnp.where(iota((mine, LANES), 1) == lane, source, 0.0), axis=1, keepdims=True
        )
        hot_count_ref[...] = jnp.sum(
            jnp.where(iota((mine, mine), 0) == iota((mine, mine), 1), column, 0.0),
            axis=0,
            keepdims=True,
        )
        everything = jnp.concatenate(
            [unfold(hot_all.at[c, n], s.piece) for c, n in order], axis=0
        )
        hot_sum_ref[...] = everything * (1.0 / jnp.sqrt(1.0 + column))

    base = rep * s.home_dev + 1

    def place_of(rows_of):
        return functools.reduce(jnp.add, rows_of).astype(jnp.int32) - base

    def tally(lab):
        high = onehot(iota((s.count_rows, LANES), 0) == (lab >> 7))
        low = onehot(iota((LANES, LANES), 0) == (lab & (LANES - 1)))
        return mm(high, low, ((1,), (1,)))

    tiles = max(1, s.home_dev // 512)
    tile = s.home_dev // tiles

    def add(q, g, first=False, last=False):
        own = range(g * s.pair, (g + 1) * s.pair)
        lab = place_of([arrived[q, p, s.block - 1 :] for p in own])
        if first:
            tally_ref[...] = tally(lab)
        elif g < s.pairs - 1:
            tally_ref[...] += tally(lab)
        blocks = [unfold(arrived.at[q, p], cap) for p in own]
        hi, lo = split(jnp.concatenate(blocks, axis=0))
        both = jnp.concatenate([hi, lo], axis=0)
        for t in range(tiles):
            here = onehot(iota((tile, LANES), 0) + t * tile == lab)
            at = pl.ds(t * tile, tile)
            total = mm(jnp.concatenate([here, here], axis=1), both)
            if not first:
                total = sum_ref[at, :] + total
            if last:
                scale = scale_ref[at, :]
                total = total * jnp.concatenate([scale] * (width // LANES), axis=1)
            sum_ref[at, :] = total

    far_half = me // (owners // 2)
    far_part = lax.rem(me // (owners // 4), 2)
    outer = 1 - lax.rem(far_half + far_part, 2)

    def pass_on(n):
        u, v = n // unit, n % unit
        inner, even, odd = (order[u] * unit + v for order in ORDERS)
        if inner == even == odd:
            p = inner
        else:
            p = inner + outer * ((even - inner) + core * (odd - even))
        for i in range(len(spans)):
            if n:
                piece = arrived.at[0, p, spans[i]]
                pltpu.make_async_copy(piece, piece, recv1.at[p, i]).wait()
            for q in range(1, reps):
                forward(q, p, i).start()

    def tags_done():
        for p in range(last_pair, owners):
            send_tag(p).wait_recv()
        for q in range(1, reps):
            pass_tags(q).start()

    def counts_done():
        count = tally_ref[...]
        for q in range(reps):
            if q:
                pass_tags(q).wait_recv()
            count = count + tally(place_of([tags_in[q, i] for i in range(s.pair)]))
        count_ref[...] = count[: s.home_rows]
        scale = 1.0 / jnp.sqrt(1.0 + count)
        for k in range(s.home_rows):
            wide = jnp.broadcast_to(scale[k : k + 1], (LANES, LANES))
            scale_ref[k * LANES : (k + 1) * LANES] = wide.T

    def peers(g, last=False):
        for q in range(1, reps):
            for p in range(g * s.pair, (g + 1) * s.pair):
                for i in range(len(spans)):
                    forward(q, p, i).wait_recv()
            add(q, g, last=last and q == reps - 1)

    feats = []

    def pack(c):
        if c == 0:
            loads[4].wait()
            feats.extend(split(feat_ref[...]))
        place = onehot(iota((width, rows), 0) + c * width == slot)
        packed = mm(place, feats[0]) + mm(place, feats[1])
        for i in range(nb):
            p = c * nb + i
            for k in range(s.parts):
                part = packed[i * cap : (i + 1) * cap, k * LANES : (k + 1) * LANES]
                block_of(p)[k * cap : (k + 1) * cap] = part

    def send(u):
        for p in range(max(1, u * unit), (u + 1) * unit):
            send_block(p)

    def follow(u):
        for p in range(u * unit, (u + 1) * unit):
            pass_on(p)

    def send_tags():
        for p in range(last_pair, owners):
            send_tag(p).start()

    def enter():
        pl.semaphore_wait(barrier, owners + reps - 2)

    steps = {
        "M": lambda n: make_tags(),
        "K": pack,
        "B": lambda n: enter(),
        "s": send,
        "f": follow,
        "t": lambda n: send_tags(),
        "T": lambda n: tags_done(),
        "C": lambda n: counts_done(),
        "a": lambda n: add(0, n, first=n == 0),
        "p": lambda n: peers(n, last=n == s.pairs - 1),
        "H": lambda n: (hot_start, hot_1, hot_2, hot_3, hot_4, hot_5, hot_6)[n](),
    }
    for step in PLAN:
        steps[step[0]](int(step[1:]))

    to_core.wait_send()
    for d in range(1, s.near):
        to_near(d).wait_send()
        to_all(d).wait_send()
    for q in range(1, reps):
        to_rep(q).wait_send()
        pass_tags(q).wait_send()
    for f in range(1, s.far):
        to_far(f).wait_send()
    to_mate.wait_send()
    pltpu.make_async_copy(tags, tags, tsend).wait()
    pltpu.make_async_copy(bucket, bucket, send1).wait()
    if reps > 1:
        sent = arrived.at[pl.ds(1, reps - 1)]
        pltpu.make_async_copy(sent, sent, send2).wait()


def write_out(*refs):
    n = len(refs) // 2
    sems = refs[-1]
    copies = [pltpu.make_async_copy(refs[i], refs[n + i], sems.at[i]) for i in range(n)]
    for copy in copies:
        copy.start()
    for copy in copies:
        copy.wait()


def local(features, group_ids, survive, home_row, hot_ids):
    rows, width = features.shape
    groups, hots = home_row.shape[0], hot_ids.shape[0]
    s = Sizes(lax.axis_size("owner"), lax.axis_size("rep"), rows, width, groups, hots)
    owners, reps = s.owners, s.reps
    vmem = pl.BlockSpec(memory_space=pltpu.VMEM)
    hbm = pl.BlockSpec(memory_space=pltpu.HBM)
    DMA = pltpu.SemaphoreType.DMA
    VM = pltpu.VMEM
    operands = (
        group_ids.reshape(1, rows),
        survive.reshape(1, rows),
        hot_ids.reshape(1, hots),
        home_row.reshape(groups // LANES, LANES),
        features,
    )
    operands = [pltpu.with_memory_space_constraint(x, pltpu.HBM) for x in operands]
    results = pl.pallas_call(
        functools.partial(kernel, s),
        out_shape=(
            pltpu.VMEM((s.home_dev, width), F32),
            pltpu.VMEM((s.home_rows, LANES), F32),
            pltpu.VMEM((hots // reps, width), F32),
            pltpu.VMEM((1, hots // reps), F32),
        ),
        in_specs=[hbm] * 5,
        out_specs=[vmem] * 4,
        scratch_shapes=[
            VM((1, rows), jnp.int32),
            VM((1, rows), jnp.int32),
            VM((1, hots), jnp.int32),
            VM((groups // LANES, LANES), jnp.int32),
            VM((rows, width), F32),
            VM((owners - 1, s.block, LANES), F32),
            VM((reps, owners, s.block, LANES), F32),
            VM((s.pair, 1, LANES), F32),
            VM((reps, s.pair, 1, LANES), F32),
            VM((s.count_rows, LANES), F32),
            VM((s.home_dev, LANES), F32),
            VM((2, s.near, reps, s.hot_block, LANES), F32),
            VM((s.near, reps, s.hot_block, LANES), F32),
            VM((s.near, reps, s.hot_block, LANES), F32),
            VM((s.near, reps, s.hot_block, LANES), F32),
            VM((reps, s.hot_block, LANES), F32),
            VM((reps, s.hot_block, LANES), F32),
            VM((s.hot_block, LANES), F32),
            VM((s.far, s.hot_block, LANES), F32),
            VM((s.hot_block, LANES), F32),
            VM((2, s.near, s.hot_block, LANES), F32),
            DMA((5,)),
            DMA(()),
            DMA((owners, 1)),
            DMA(()),
            DMA((reps, owners, 1)),
            DMA(()),
            DMA((s.pair,)),
            DMA(()),
            DMA((reps,)),
            DMA((6,)),
            DMA(()),
            DMA((s.near,)),
            DMA((reps,)),
            DMA((s.far,)),
            DMA((s.near,)),
            DMA(()),
        ],
        compiler_params=pltpu.CompilerParams(
            collective_id=0, has_side_effects=True, vmem_limit_bytes=48 << 20
        ),
    )(*operands)
    results = [pltpu.with_memory_space_constraint(x, pltpu.VMEM) for x in results]
    cold_sum, count, hot_sum, hot_count = pl.pallas_call(
        write_out,
        out_shape=[jax.ShapeDtypeStruct(x.shape, x.dtype) for x in results],
        in_specs=[vmem] * 4,
        out_specs=[hbm] * 4,
        scratch_shapes=[DMA((4,))],
    )(*results)
    return cold_sum, count.reshape(s.home_dev), hot_sum, hot_count.reshape(hots // reps)


def solution(mesh):
    in_specs = (P(("owner", "rep"), None), P(("owner", "rep")), P(("owner", "rep")), P(), P())
    out_specs = (P(("owner", "rep"), None), P(("owner", "rep")), P("rep", None), P("rep"))
    return jax.shard_map(local, mesh=mesh, in_specs=in_specs, out_specs=out_specs, check_vma=False)
```

```python
import functools

import jax
import jax.numpy as jnp
from jax import lax
from jax.experimental import pallas as pl
from jax.experimental.pallas import tpu as pltpu
from jax.sharding import PartitionSpec as P

MESH = pl.DeviceIdType.MESH
LANES = 128
SUB = 8
BF = jnp.bfloat16
F32 = jnp.float32


def iota(shape, axis):
    return lax.broadcasted_iota(jnp.int32, shape, axis)


def mm(a, b, dims=((1,), (0,))):
    return lax.dot_general(a, b, (dims, ((), ())), preferred_element_type=F32)


def split(x):
    hi = x.astype(BF)
    return hi, (x - hi.astype(F32)).astype(BF)


def onehot(mask):
    return jnp.where(mask, 1.0, 0.0).astype(BF)


def log2(n):
    return n.bit_length() - 1


PLAN = (
    "M0", "K0", "B0", "s1", "s3", "s2", "f0", "t0", "K1", "s4", "H0", "s5",
    "s6", "s7", "K2", "s8", "s9", "s10", "K3", "f1", "H1", "s11", "s13", "f2",
    "f3", "f4", "f5", "f6", "s12", "f7", "T0", "a0", "a1", "H2", "f8", "f9",
    "H3", "s14", "s15", "f10", "f11", "a2", "a3", "p0", "f12", "a4", "f13", "H4",
    "p1", "f14", "f15", "a5", "a6", "p2", "p4", "p3", "p5", "H5", "p6", "a7",
    "C0", "H6", "p7",
)

ORDERS = (
    (0, 1, 3, 2, 4, 5, 9, 6, 7, 8, 10, 11, 12, 13, 14, 15),
    (0, 1, 2, 8, 3, 9, 10, 11, 4, 5, 6, 7, 12, 13, 15, 14),
    (0, 1, 2, 8, 3, 10, 4, 9, 5, 6, 7, 12, 13, 11, 14, 15),
)


class Sizes:
    def __init__(self, owners, reps, rows, width, groups, hots):
        self.owners, self.reps, self.rows, self.width, self.hots = owners, reps, rows, width, hots
        self.groups = groups
        self.own_groups = groups // owners
        self.home_dev = self.own_groups // reps
        self.cap = 2 * rows // owners
        self.nb = width // self.cap
        self.pair = LANES // self.cap
        self.pairs = owners // self.pair
        self.chips = owners // 2
        self.part = hots // reps // 2
        self.near = min(self.chips // 2, self.part // SUB)
        self.far = self.chips // self.near
        self.piece = self.part // self.near
        self.home_rows = self.home_dev // LANES
        self.parts = width // LANES
        self.block = self.parts * self.cap + 1
        self.hot_block = self.parts * self.piece + 1
        self.count_rows = max(SUB, self.home_rows)


def kernel(
    s,
    ids_hbm,
    survive_hbm,
    hot_hbm,
    table_hbm,
    feat_hbm,
    sum_ref,
    count_ref,
    hot_sum_ref,
    hot_count_ref,
    ids_ref,
    survive_ref,
    hot_ref,
    table_ref,
    feat_ref,
    bucket,
    arrived,
    tags,
    tags_in,
    tally_ref,
    scale_ref,
    hot_part,
    hot_l1,
    hot_s1,
    hot_l2,
    hot_s2,
    hot_l3,
    hot_s3,
    hot_l4,
    hot_s4,
    hot_all,
    load,
    send1,
    recv1,
    send2,
    recv2,
    tsend,
    trecv,
    tsend2,
    trecv2,
    hsend,
    h_core,
    h_near,
    h_rep,
    h_far,
    h_all,
    h_last,
):
    owners, reps, cap, nb = s.owners, s.reps, s.cap, s.nb
    unit = s.pair // 2
    rows, width, hots = s.rows, s.width, s.hots
    me = lax.axis_index("owner")
    rep = lax.axis_index("rep")
    core = lax.rem(me, 2)
    near = lax.rem(me // 2, s.near)

    loads = [
        pltpu.make_async_copy(src, dst, load.at[i])
        for i, (src, dst) in enumerate(
            (
                (table_hbm, table_ref),
                (ids_hbm, ids_ref),
                (survive_hbm, survive_ref),
                (hot_hbm, hot_ref),
                (feat_hbm, feat_ref),
            )
        )
    ]
    for copy in loads:
        copy.start()

    barrier = pltpu.get_barrier_semaphore()

    @pl.loop(1, owners)
    def _(d):
        pl.semaphore_signal(
            barrier, inc=1, device_id=(lax.rem(me + d, owners), rep), device_id_type=MESH
        )

    @pl.loop(1, reps)
    def _(d):
        pl.semaphore_signal(
            barrier, inc=1, device_id=(me, lax.rem(rep + d, reps)), device_id_type=MESH
        )

    flips = []
    bit = 1
    while bit < owners:
        flips.append((bit, bit - 2 * bit * lax.rem(me // bit, 2)))
        bit *= 2

    def partner(p):
        out = me
        for bit, flip in flips:
            if p & bit:
                out = out + flip
        return out

    def other_rep(q):
        return lax.rem(rep + q, reps)

    def remote(src, dst, send, recv, device):
        return pltpu.make_async_remote_copy(
            src_ref=src,
            dst_ref=dst,
            send_sem=send,
            recv_sem=recv,
            device_id=device,
            device_id_type=MESH,
        )

    for copy in loads[:4]:
        copy.wait()
    ids = ids_ref[...]
    live_f = jnp.where(survive_ref[...] == 1, 1.0, 0.0)
    table = table_ref[...]
    trows = table.shape[0]
    halves = jnp.concatenate([table >> 8, table & 255], axis=1).astype(F32).astype(BF)
    pick = onehot(iota((trows, rows), 0) == (ids >> 7))
    both = mm(halves, pick, ((0,), (0,)))
    column = both[:LANES] * 256.0 + both[LANES:]
    home = jnp.sum(
        jnp.where(iota((LANES, rows), 0) == (ids & (LANES - 1)), column, 0.0), axis=0, keepdims=True
    )
    target = jnp.floor(home * (1.0 / s.own_groups))
    label = home - target * s.own_groups + 1.0
    place_at = target.astype(jnp.int32) ^ me

    at = iota((hots, hots), 0)
    block = at >> log2(s.piece)
    number = (
        (block & (reps - 1)) * (2 * s.part)
        + (block >> log2(reps)) * s.piece
        + (at & (s.piece - 1))
    )
    hot_col = jnp.sum(
        jnp.where(number == iota((hots, hots), 1), hot_ref[...].astype(F32), 0.0),
        axis=1,
        keepdims=True,
    )
    matches = jnp.where(hot_col == ids.astype(F32), 1.0, 0.0)
    is_hot = jnp.max(matches, axis=0, keepdims=True)
    keep = live_f * (1.0 - is_hot)
    place_at = jnp.where(keep > 0.0, place_at, -1)

    member = jnp.where(iota((owners, rows), 0) == place_at, 1.0, 0.0)
    before = onehot(iota((rows, rows), 0) < iota((rows, rows), 1))
    position = mm(member.astype(BF), before)
    placed = jnp.sum(position * member, axis=0, keepdims=True).astype(jnp.int32)
    slot = jnp.where(keep > 0.0, place_at * cap + placed, -1)

    last_pair = owners - s.pair

    def make_tags():
        lane = placed + cap * (place_at & (s.pair - 1))
        label_hi = jnp.floor(label * (1.0 / 256.0))
        label_lo = label - 256.0 * label_hi
        coded = jnp.concatenate([member * label_hi, member * label_lo], axis=0).astype(BF)
        where = onehot(iota((LANES, rows), 0) == lane)
        coded = mm(coded, where, ((1,), (1,)))
        labels = coded[:owners] * 256.0 + coded[owners:]
        for p in range(owners):
            block_of(p)[s.block - 1 :] = labels[p : p + 1]
        for p in range(last_pair, owners):
            tags[p - last_pair] = labels[p : p + 1]

    def block_of(p):
        return arrived.at[0, 0] if p == 0 else bucket.at[p - 1]

    def unfold(ref, n):
        return jnp.concatenate([ref[k * n : (k + 1) * n] for k in range(s.parts)], axis=1)

    spans = (pl.ds(0, s.block),)

    def send_block(p):
        for i, span in enumerate(spans):
            remote(
                bucket.at[p - 1, span],
                arrived.at[0, p, span],
                send1,
                recv1.at[p, i],
                (partner(p), rep),
            ).start()

    def forward(q, p, i):
        piece = arrived.at[0, p, spans[i]]
        return remote(
            piece, arrived.at[q, p, spans[i]], send2, recv2.at[q, p, i], (me, other_rep(q))
        )

    def send_tag(p):
        i = p - last_pair
        return remote(tags.at[i], tags_in.at[0, i], tsend, trecv.at[i], (partner(p), rep))

    def pass_tags(q):
        return remote(tags_in.at[0], tags_in.at[q], tsend2, trecv2.at[q], (me, other_rep(q)))

    mate = (partner(1), rep)
    to_core = remote(hot_part.at[1 - core], hot_l1, hsend.at[0], h_core, mate)

    def to_near(d):
        there = partner(2 * d)
        index = lax.rem(there // 2, s.near)
        return remote(hot_s1.at[index], hot_l2.at[d], hsend.at[1], h_near.at[d], (there, rep))

    def to_rep(q):
        return remote(
            hot_s2.at[other_rep(q)], hot_l3.at[q], hsend.at[2], h_rep.at[q], (me, other_rep(q))
        )

    def to_far(f):
        return remote(
            hot_s3, hot_l4.at[f], hsend.at[3], h_far.at[f], (partner(2 * s.near * f), rep)
        )

    def to_all(d):
        return remote(
            hot_s4, hot_all.at[core, near], hsend.at[4], h_all.at[near], (partner(2 * d), rep)
        )

    def from_all(d):
        index = lax.rem(partner(2 * d) // 2, s.near)
        piece = hot_all.at[core, index]
        return pltpu.make_async_copy(piece, piece, h_all.at[index])

    to_mate = remote(hot_all.at[core], hot_all.at[core], hsend.at[5], h_last, mate)

    def hot_start():
        hot_bf = (matches * live_f).astype(BF)
        sums = mm(hot_bf, feats[0]) + mm(hot_bf, feats[1])
        lives = jnp.broadcast_to(live_f, (SUB, rows)).astype(BF)
        counts = mm(lives, hot_bf, ((1,), (1,)))[:1]
        shape = (2, s.near, reps, s.piece, LANES)
        for k in range(s.parts):
            part = sums[:, k * LANES : (k + 1) * LANES].reshape(shape)
            hot_part[:, :, :, k * s.piece : (k + 1) * s.piece] = part
        half = hots // 2
        for c in range(2):
            for n in range(s.near):
                for r in range(reps):
                    hot_part[c, n, r, s.hot_block - 1 :] = counts[:, c * half : (c + 1) * half]
        to_core.start()

    def hot_1():
        to_core.wait_recv()
        hot_s1[...] = hot_part[core] + hot_l1[...]
        for d in range(1, s.near):
            to_near(d).start()

    def hot_2():
        total = hot_s1[near]
        for d in range(1, s.near):
            to_near(d).wait_recv()
            total = total + hot_l2[d]
        hot_s2[...] = total
        for q in range(1, reps):
            to_rep(q).start()

    def hot_3():
        total = hot_s2[rep]
        for q in range(1, reps):
            to_rep(q).wait_recv()
            total = total + hot_l3[q]
        hot_s3[...] = total
        for f in range(1, s.far):
            to_far(f).start()

    def hot_4():
        total = hot_s3[...]
        for f in range(1, s.far):
            to_far(f).wait_recv()
            total = total + hot_l4[f]
        hot_s4[...] = total
        hot_all[core, near] = total
        for d in range(1, s.near):
            to_all(d).start()

    def hot_5():
        for d in range(1, s.near):
            from_all(d).wait()
        to_mate.start()

    def hot_6():
        to_mate.wait_recv()
        mine = hots // reps
        order = [(c, n) for c in range(2) for n in range(s.near)]
        source = jnp.concatenate(
            [
                jnp.broadcast_to(hot_all[c, n, s.hot_block - 1 :], (s.piece, LANES))
                for c, n in order
            ],
            axis=0,
        )
        j = iota((mine, LANES), 0)
        lane = (
            ((j & (s.part - 1)) >> log2(s.piece)) * (reps * s.piece)
            + rep * s.piece
            + (j & (s.piece - 1))
        )
        column = jnp.sum(
            jnp.where(iota((mine, LANES), 1) == lane, source, 0.0), axis=1, keepdims=True
        )
        hot_count_ref[...] = jnp.sum(
            jnp.where(iota((mine, mine), 0) == iota((mine, mine), 1), column, 0.0),
            axis=0,
            keepdims=True,
        )
        everything = jnp.concatenate(
            [unfold(hot_all.at[c, n], s.piece) for c, n in order], axis=0
        )
        hot_sum_ref[...] = everything * (1.0 / jnp.sqrt(1.0 + column))

    base = rep * s.home_dev + 1

    def place_of(rows_of):
        return functools.reduce(jnp.add, rows_of).astype(jnp.int32) - base

    def tally(lab):
        high = onehot(iota((s.count_rows, LANES), 0) == (lab >> 7))
        low = onehot(iota((LANES, LANES), 0) == (lab & (LANES - 1)))
        return mm(high, low, ((1,), (1,)))

    tiles = max(1, s.home_dev // 512)
    tile = s.home_dev // tiles

    def add(q, g, first=False, last=False):
        own = range(g * s.pair, (g + 1) * s.pair)
        lab = place_of([arrived[q, p, s.block - 1 :] for p in own])
        if first:
            tally_ref[...] = tally(lab)
        elif g < s.pairs - 1:
            tally_ref[...] += tally(lab)
        blocks = [unfold(arrived.at[q, p], cap) for p in own]
        hi, lo = split(jnp.concatenate(blocks, axis=0))
        both = jnp.concatenate([hi, lo], axis=0)
        for t in range(tiles):
            here = onehot(iota((tile, LANES), 0) + t * tile == lab)
            at = pl.ds(t * tile, tile)
            total = mm(jnp.concatenate([here, here], axis=1), both)
            if not first:
                total = sum_ref[at, :] + total
            if last:
                scale = scale_ref[at, :]
                total = total * jnp.concatenate([scale] * (width // LANES), axis=1)
            sum_ref[at, :] = total

    far_half = me // (owners // 2)
    far_part = lax.rem(me // (owners // 4), 2)
    outer = 1 - lax.rem(far_half + far_part, 2)

    def pass_on(n):
        u, v = n // unit, n % unit
        inner, even, odd = (order[u] * unit + v for order in ORDERS)
        if inner == even == odd:
            p = inner
        else:
            p = inner + outer * ((even - inner) + core * (odd - even))
        for i in range(len(spans)):
            if n:
                piece = arrived.at[0, p, spans[i]]
                pltpu.make_async_copy(piece, piece, recv1.at[p, i]).wait()
            for q in range(1, reps):
                forward(q, p, i).start()

    def tags_done():
        for p in range(last_pair, owners):
            send_tag(p).wait_recv()
        for q in range(1, reps):
            pass_tags(q).start()

    def counts_done():
        count = tally_ref[...]
        for q in range(reps):
            if q:
                pass_tags(q).wait_recv()
            count = count + tally(place_of([tags_in[q, i] for i in range(s.pair)]))
        count_ref[...] = count[: s.home_rows]
        scale = 1.0 / jnp.sqrt(1.0 + count)
        for k in range(s.home_rows):
            wide = jnp.broadcast_to(scale[k : k + 1], (LANES, LANES))
            scale_ref[k * LANES : (k + 1) * LANES] = wide.T

    def peers(g, last=False):
        for q in range(1, reps):
            for p in range(g * s.pair, (g + 1) * s.pair):
                for i in range(len(spans)):
                    forward(q, p, i).wait_recv()
            add(q, g, last=last and q == reps - 1)

    feats = []

    def pack(c):
        if c == 0:
            loads[4].wait()
            feats.extend(split(feat_ref[...]))
        place = onehot(iota((width, rows), 0) + c * width == slot)
        packed = mm(place, feats[0]) + mm(place, feats[1])
        for i in range(nb):
            p = c * nb + i
            for k in range(s.parts):
                part = packed[i * cap : (i + 1) * cap, k * LANES : (k + 1) * LANES]
                block_of(p)[k * cap : (k + 1) * cap] = part

    def send(u):
        for p in range(max(1, u * unit), (u + 1) * unit):
            send_block(p)

    def follow(u):
        for p in range(u * unit, (u + 1) * unit):
            pass_on(p)

    def send_tags():
        for p in range(last_pair, owners):
            send_tag(p).start()

    def enter():
        pl.semaphore_wait(barrier, owners + reps - 2)

    steps = {
        "M": lambda n: make_tags(),
        "K": pack,
        "B": lambda n: enter(),
        "s": send,
        "f": follow,
        "t": lambda n: send_tags(),
        "T": lambda n: tags_done(),
        "C": lambda n: counts_done(),
        "a": lambda n: add(0, n, first=n == 0),
        "p": lambda n: peers(n, last=n == s.pairs - 1),
        "H": lambda n: (hot_start, hot_1, hot_2, hot_3, hot_4, hot_5, hot_6)[n](),
    }
    for step in PLAN:
        steps[step[0]](int(step[1:]))

    to_core.wait_send()
    for d in range(1, s.near):
        to_near(d).wait_send()
        to_all(d).wait_send()
    for q in range(1, reps):
        to_rep(q).wait_send()
        pass_tags(q).wait_send()
    for f in range(1, s.far):
        to_far(f).wait_send()
    to_mate.wait_send()
    pltpu.make_async_copy(tags, tags, tsend).wait()
    pltpu.make_async_copy(bucket, bucket, send1).wait()
    if reps > 1:
        sent = arrived.at[pl.ds(1, reps - 1)]
        pltpu.make_async_copy(sent, sent, send2).wait()


def write_out(*refs):
    n = len(refs) // 2
    sems = refs[-1]
    copies = [pltpu.make_async_copy(refs[i], refs[n + i], sems.at[i]) for i in range(n)]
    for copy in copies:
        copy.start()
    for copy in copies:
        copy.wait()


def local(features, group_ids, survive, home_row, hot_ids):
    rows, width = features.shape
    groups, hots = home_row.shape[0], hot_ids.shape[0]
    s = Sizes(lax.axis_size("owner"), lax.axis_size("rep"), rows, width, groups, hots)
    owners, reps = s.owners, s.reps
    vmem = pl.BlockSpec(memory_space=pltpu.VMEM)
    hbm = pl.BlockSpec(memory_space=pltpu.HBM)
    DMA = pltpu.SemaphoreType.DMA
    VM = pltpu.VMEM
    operands = (
        group_ids.reshape(1, rows),
        survive.reshape(1, rows),
        hot_ids.reshape(1, hots),
        home_row.reshape(groups // LANES, LANES),
        features,
    )
    operands = [pltpu.with_memory_space_constraint(x, pltpu.HBM) for x in operands]
    results = pl.pallas_call(
        functools.partial(kernel, s),
        out_shape=(
            pltpu.VMEM((s.home_dev, width), F32),
            pltpu.VMEM((s.home_rows, LANES), F32),
            pltpu.VMEM((hots // reps, width), F32),
            pltpu.VMEM((1, hots // reps), F32),
        ),
        in_specs=[hbm] * 5,
        out_specs=[vmem] * 4,
        scratch_shapes=[
            VM((1, rows), jnp.int32),
            VM((1, rows), jnp.int32),
            VM((1, hots), jnp.int32),
            VM((groups // LANES, LANES), jnp.int32),
            VM((rows, width), F32),
            VM((owners - 1, s.block, LANES), F32),
            VM((reps, owners, s.block, LANES), F32),
            VM((s.pair, 1, LANES), F32),
            VM((reps, s.pair, 1, LANES), F32),
            VM((s.count_rows, LANES), F32),
            VM((s.home_dev, LANES), F32),
            VM((2, s.near, reps, s.hot_block, LANES), F32),
            VM((s.near, reps, s.hot_block, LANES), F32),
            VM((s.near, reps, s.hot_block, LANES), F32),
            VM((s.near, reps, s.hot_block, LANES), F32),
            VM((reps, s.hot_block, LANES), F32),
            VM((reps, s.hot_block, LANES), F32),
            VM((s.hot_block, LANES), F32),
            VM((s.far, s.hot_block, LANES), F32),
            VM((s.hot_block, LANES), F32),
            VM((2, s.near, s.hot_block, LANES), F32),
            DMA((5,)),
            DMA(()),
            DMA((owners, 1)),
            DMA(()),
            DMA((reps, owners, 1)),
            DMA(()),
            DMA((s.pair,)),
            DMA(()),
            DMA((reps,)),
            DMA((6,)),
            DMA(()),
            DMA((s.near,)),
            DMA((reps,)),
            DMA((s.far,)),
            DMA((s.near,)),
            DMA(()),
        ],
        compiler_params=pltpu.CompilerParams(
            collective_id=0, has_side_effects=True, vmem_limit_bytes=48 << 20
        ),
    )(*operands)
    results = [pltpu.with_memory_space_constraint(x, pltpu.VMEM) for x in results]
    cold_sum, count, hot_sum, hot_count = pl.pallas_call(
        write_out,
        out_shape=[jax.ShapeDtypeStruct(x.shape, x.dtype) for x in results],
        in_specs=[vmem] * 4,
        out_specs=[hbm] * 4,
        scratch_shapes=[DMA((4,))],
    )(*results)
    return cold_sum, count.reshape(s.home_dev), hot_sum, hot_count.reshape(hots // reps)


def solution(mesh):
    in_specs = (P(("owner", "rep"), None), P(("owner", "rep")), P(("owner", "rep")), P(), P())
    out_specs = (P(("owner", "rep"), None), P(("owner", "rep")), P("rep", None), P("rep"))
    return jax.shard_map(local, mesh=mesh, in_specs=in_specs, out_specs=out_specs, check_vma=False)
```
